32 devices in a mesh: real: 2 (over x), row: 16 (over z, y, core).
Axes of the slice: x: 2, y: 2, z: 4, core: 2. Of those that a mesh axis runs over, the one named last changes fastest.
Arguments:
- site_tensor: float32 [32, 2, 256, 256], P(('real', 'row')), parts along dimension 0, may hold values from -20 to 20
- left_env: float32 [32, 14, 256, 256], P(('real', 'row')), parts along dimension 0, may hold values from -10 to 10
- right_env: float32 [32, 14, 256, 256], P(('real', 'row')), parts along dimension 0, may hold values from -10 to 10
- sector_size: int32 [32], P('real'), parts along dimension 0, may hold values from 64 to 256
Outputs:
- left_out: float32 [32, 2, 256, 256], P(('real', 'row')), parts along dimension 0
- bond_out: float32 [32, 256, 256], P(('real', 'row')), parts along dimension 0
The draws below stay inside these ranges and needn't reach their ends.
There are 2 independent parts, one for each index of `real`. The reference program is written for one: setup_inputs(seed, part) draws one part's arguments, and reference() takes and returns one part's arrays. A program takes and returns all parts, laid end to end along the dimension named above; each array names one. Nothing has to cross between parts.
All inputs are finite; a program needn't handle non-finite values.
Results may differ from the reference program's by a relative error of at most 0.00005.
Values sent between devices are 32-bit elements; how exact they have to be, the bound alone decides.
A program may use at most 64 MiB of HBM per device.

```python
import jax
import jax.numpy as jnp
from jax import lax

SEC = 256
W_DN = 4
W_UP = 4
W = 14
SECTORS = 16


def sector_ramp(total_rise):
    position = jnp.arange(SECTORS, dtype=jnp.float32) / max(SECTORS - 1, 1)
    return jnp.exp(jnp.log(total_rise) * position)


def draw_site_tensor(key, part):
    key_noise, key_scale = jax.random.split(jax.random.fold_in(key, 11))
    random_part = jnp.clip(jax.random.normal(key_noise, (SECTORS, 2, SEC, SEC), jnp.float32), -6.0, 6.0)
    column_scale = jnp.exp(jnp.clip(0.2 * jax.random.normal(key_scale, (SECTORS, 2, 1, SEC), jnp.float32), -0.8, 0.8))
    ramp = jnp.sqrt(sector_ramp(3.0))
    random_part = random_part * SEC ** (-0.5)
    identity = jnp.eye(SEC, dtype=jnp.float32)
    upper_block = identity[None] + 0.35 * random_part[:, 0]
    lower_block = 0.7 * random_part[:, 1]
    return jnp.stack([upper_block, lower_block], 1) * column_scale * ramp[:, None, None, None]


def environment_noise(key):
    noise = jnp.clip(jax.random.normal(key, (SECTORS, W, SEC, SEC), jnp.float32), -6.0, 6.0)
    return noise * SEC ** (-0.5)


def draw_left_env(key, part):
    key_noise, key_field = jax.random.split(jax.random.fold_in(key, 23))
    noise = environment_noise(key_noise)
    rough = jnp.exp(jax.random.uniform(key_field, (SECTORS, SEC), jnp.float32, jnp.log(0.5), jnp.log(2.0)))
    ramp = sector_ramp(3.0)
    field = rough * ramp[:, None]
    identity = jnp.eye(SEC, dtype=jnp.float32)
    onsite = field[:, :, None] * identity[None]
    return noise.at[:, W - 1].add(onsite)


def draw_right_env(key, part):
    noise = environment_noise(jax.random.fold_in(key, 37))
    identity = jnp.eye(SEC, dtype=jnp.float32)
    return noise.at[:, W - 1].add(identity[None])


def with_ends(values, own_key, least, high):
    dims = values.shape
    index_at = [jax.random.randint(jax.random.fold_in(own_key, axis), (), 0, dims[axis]) for axis in range(len(dims))]
    values = values.at[tuple(index_at)].set(least)
    longest = dims.index(max(dims))
    index_at[longest] = (index_at[longest] + 1) % dims[longest]
    return values.at[tuple(index_at)].set(high)


def setup_inputs(seed: int = 0, part: int = 0) -> dict:
    seeds = jax.random.split(jax.random.key(seed), 5)
    part_keys = jax.random.split(jax.random.fold_in(seeds[4], part), 5)
    site_tensor = draw_site_tensor(jax.random.fold_in(jax.random.fold_in(seeds[4], part), 71), part)
    left_env = draw_left_env(jax.random.fold_in(jax.random.fold_in(seeds[4], part), 71), part)
    right_env = draw_right_env(jax.random.fold_in(jax.random.fold_in(seeds[4], part), 71), part)
    sector_size = with_ends(jax.random.randint(part_keys[3], (SECTORS,), SEC // 4, SEC + 1), jax.random.fold_in(part_keys[3], 1), SEC // 4, SEC).astype(jnp.int32)
    return {"site_tensor": site_tensor, "left_env": left_env, "right_env": right_env, "sector_size": sector_size}


highest = lax.Precision.HIGHEST
time_step = 0.15

def solve_rows(factor, stacked):
    return jax.scipy.linalg.solve_triangular(factor, stacked.T, lower=True).T

def apply_bond(operand, left_env, right_env, mask_pair):
    products = jnp.einsum('sik,sakl->sail', operand, right_env, precision=highest)
    empty_block = jnp.zeros_like(products[:1])
    down_terms = jnp.concatenate([empty_block[:, :W_DN], products[:-1, :W_DN]], 0)
    upper_terms = jnp.concatenate([products[1:, W_DN:W_DN + W_UP], empty_block[:, W_DN:W_DN + W_UP]], 0)
    combined = jnp.concatenate([down_terms, upper_terms, products[:, W_DN + W_UP:]], 1)
    return jnp.einsum('saij,sajl->sil', left_env, combined, precision=highest) * mask_pair

def reference(site_tensor, left_env, right_env, sector_size):
    live_mask = (jnp.arange(SEC, dtype=jnp.int32)[None, :] < sector_size[:, None]).astype(jnp.float32)
    row_mask = live_mask[:, :, None]
    col_mask = live_mask[:, None, :]
    mask_pair = row_mask * col_mask
    upper_block = site_tensor[:, 0] * mask_pair
    lower_source = site_tensor[:, 1] * row_mask
    lower_block = jnp.concatenate([jnp.zeros_like(lower_source[:1]), lower_source[:-1]], 0) * col_mask
    stacked = jnp.concatenate([upper_block, lower_block], 1)
    identity = jnp.eye(SEC, dtype=jnp.float32)
    gram_matrix = jnp.einsum('sij,sik->sjk', stacked, stacked, precision=highest) + identity[None] * (1.0 - live_mask)[:, None, :]
    factor = jnp.linalg.cholesky(gram_matrix)
    orthonormal = jax.vmap(solve_rows)(factor, stacked)
    moved_back = jnp.concatenate([orthonormal[1:, SEC:], jnp.zeros_like(orthonormal[:1, SEC:])], 0)
    left_out = jnp.stack([orthonormal[:, :SEC], moved_back], 1)
    bond_matrix = jnp.swapaxes(factor, 1, 2) * mask_pair
    start_norm = jnp.sum(bond_matrix * bond_matrix)
    applied = apply_bond(bond_matrix, left_env, right_env, mask_pair)
    energy = jnp.sum(bond_matrix * applied) / start_norm
    shifted = applied - energy * bond_matrix
    second = apply_bond(shifted, left_env, right_env, mask_pair) - energy * shifted
    evolved = bond_matrix + time_step * shifted + 0.5 * time_step * time_step * second
    final_norm = jnp.sum(evolved * evolved)
    return (left_out, evolved * jnp.sqrt(start_norm / final_norm))
```

```python
import functools

import jax
import jax.numpy as jnp
from jax import lax
from jax.experimental import pallas as pl
from jax.experimental.pallas import tpu as pltpu
from jax.sharding import PartitionSpec as P

W_DN = 4
W_UP = 4
PANEL = 16
TAU = 0.15
highest = lax.Precision.HIGHEST
f32 = jnp.float32
bf16 = jnp.bfloat16
MESH = pl.DeviceIdType.MESH


def dot(a, b):
    return jnp.dot(a, b, preferred_element_type=f32)


def split_2(value):
    high = value.astype(bf16)
    return high, (value - high.astype(f32)).astype(bf16)


def split_3(value):
    high = value.astype(bf16)
    rest = value - high.astype(f32)
    middle = rest.astype(bf16)
    return high, middle, (rest - middle.astype(f32)).astype(bf16)


def store_split(pair_ref, index, value):
    high, low = split_2(value)
    pair_ref[0, index] = high
    pair_ref[1, index] = low


def tile_sum(value):
    rows, columns = value.shape
    summed = jnp.sum(value.reshape(rows // 8, 8, columns), axis=0)
    total = summed[:, :128]
    for start in range(128, columns, 128):
        total = total + summed[:, start : start + 128]
    return total


def full_sum(tile):
    return jnp.sum(jnp.sum(tile, axis=0, keepdims=True), axis=1, keepdims=True)


def panel_step(p, lo, hi, states, aug_ref, out_ref):
    base = pl.multiple_of(p * PANEL, PANEL)
    row_id = lax.broadcasted_iota(jnp.int32, (PANEL, 128), 0)
    offset = lax.rem(p * PANEL, 128)
    diag = aug_ref[pl.ds(base, PANEL), lo : lo + 128]
    diag = pltpu.roll(diag, lax.rem(128 - offset, 128), 1)
    columns = [jnp.broadcast_to(diag[:, r : r + 1], (PANEL, 128)) for r in range(PANEL)]
    tiles = [aug_ref[pl.ds(base, PANEL), t : t + 128] for t in range(lo, hi, 128)]
    scale = jnp.zeros((PANEL, 128), f32)
    for r in range(PANEL):
        inverse = lax.rsqrt(columns[r][r : r + 1, :])
        scale = jnp.where(row_id == r, inverse, scale)
        multiplier = columns[r] * inverse
        below = jnp.where(row_id > r, multiplier, 0.0)
        for s in range(r + 1, PANEL):
            columns[s] = columns[s] - below * multiplier[s : s + 1, :]
        if r < PANEL - 1:
            tiles = [tile - below * (tile[r : r + 1, :] * inverse) for tile in tiles]
    tiles = [tile * scale for tile in tiles]
    for t, tile in zip(range(lo, hi, 128), tiles):
        out_ref[pl.ds(base, PANEL), t : t + 128] = tile
    panel = jnp.concatenate(tiles, 1)
    q1, q2, q3 = split_3(panel)
    p1, p2, p3 = (q[:, : states - lo] for q in (q1, q2, q3))
    left = jnp.concatenate([p1, p1, p2, p2, p1, p3], 0)
    right = jnp.concatenate([q1, q2, q1, q2, q3, q1], 0)
    update = lax.dot_general(left, right, (((0,), (0,)), ((), ())), preferred_element_type=f32)
    aug_ref[lo:states, lo:hi] -= update


def kernel(
    size_ref, site_hbm, left_hbm, right_hbm,
    out_hbm, bond_out,
    site, low, left_f, right_f, left_s, right_s, aug, fac, bond, applied, acc, field_in, low_out, up_out,
    red_in, red_own, local_sem, send_sem, recv_sem, red_send, red_recv,
):
    count = lax.axis_size("row")
    me = lax.axis_index("row")
    states = site.shape[-1]
    channels = left_f.shape[0]
    moved = W_DN + W_UP
    not_first, not_last = me > 0, me < count - 1

    loads = [
        pltpu.make_async_copy(site_hbm.at[0], site, local_sem.at[0]),
        pltpu.make_async_copy(left_hbm.at[0], left_f, local_sem.at[1]),
        pltpu.make_async_copy(right_hbm.at[0, moved:], right_f.at[moved:], local_sem.at[2]),
    ]
    for load in loads:
        load.start()

    barrier = pltpu.get_barrier_semaphore()
    for step in range(1, count):
        peer = lax.rem(me + step, count)
        pl.semaphore_signal(barrier, inc=1, device_id={"row": peer}, device_id_type=MESH)
    pl.semaphore_wait(barrier, count - 1)

    def remote(source, target, slot, peer):
        return pltpu.make_async_remote_copy(
            src_ref=source, dst_ref=target, send_sem=send_sem.at[slot], recv_sem=recv_sem.at[slot],
            device_id={"row": peer}, device_id_type=MESH,
        )

    to_right, to_left = jnp.minimum(me + 1, count - 1), jnp.maximum(me - 1, 0)
    send_site = remote(site_hbm.at[0, 1], low, 0, to_right)
    send_down = remote(right_hbm.at[0, :W_DN], right_f.at[:W_DN], 1, to_right)
    send_up = remote(right_hbm.at[0, W_DN:moved], right_f.at[W_DN:moved], 2, to_left)
    send_low = remote(low_out, out_hbm.at[0, 1], 3, to_left)
    fields = [bond, applied]
    send_fields = [
        (remote(fields[t], field_in.at[t, 0], 4 + 2 * t, to_right), remote(fields[t], field_in.at[t, 1], 5 + 2 * t, to_left))
        for t in range(2)
    ]

    @pl.when(not_last)
    def _():
        send_site.start()
        send_down.start()

    @pl.when(not_first)
    def _():
        send_up.start()

    @pl.when(me == 0)
    def _():
        low[...] = jnp.zeros_like(low)
        right_f[:W_DN] = jnp.zeros((W_DN, states, states), f32)
        field_in[:, 0] = jnp.zeros((2, states, states), f32)

    @pl.when(me == count - 1)
    def _():
        right_f[W_DN:moved] = jnp.zeros((W_UP, states, states), f32)
        field_in[:, 1] = jnp.zeros((2, states, states), f32)

    size = size_ref[me]
    size_before = size_ref[to_left]
    row = lax.broadcasted_iota(jnp.int32, (states, states), 0)
    column = lax.broadcasted_iota(jnp.int32, (states, states), 1)
    live_pair = (row < size) & (column < size)
    gram_dims = (((0,), (0,)), ((), ()))
    loads[0].wait()
    upper = jnp.where(live_pair, site[0], 0.0)
    site[0] = upper
    gram = lax.dot_general(upper, upper, gram_dims, precision=highest, preferred_element_type=f32)
    gram = gram + jnp.where((row == column) & (row >= size), 1.0, 0.0)
    aug[:, states:] = jnp.where(row == column, 1.0, 0.0).astype(f32)

    @pl.when(not_first)
    def _():
        send_site.wait_recv()

    lower = jnp.where((row < size_before) & (column < size), low[...], 0.0)
    site[1] = lower
    aug[:, :states] = gram + lax.dot_general(lower, lower, gram_dims, precision=highest, preferred_element_type=f32)
    fac[...] = jnp.zeros_like(fac)
    loads[1].wait()
    loads[2].wait()

    half = states // 2
    halves = half // PANEL

    def first_half(p, carry):
        panel_step(p, 0, states + half, states, aug, fac)
        store_split(left_s, p, left_f[p])
        return carry

    def second_half(p, carry):
        panel_step(p, half, 2 * states, states, aug, fac)
        other = jnp.minimum(p, channels - 1)
        store_split(left_s, other, left_f[other])
        mine = jnp.minimum(p - halves + moved, channels - 1)
        store_split(right_s, mine, right_f[mine])
        return carry

    lax.fori_loop(0, halves, first_half, 0)
    lax.fori_loop(halves, 2 * halves, second_half, 0)

    bond[...] = jnp.where(live_pair & (column >= row), fac[:, :states], 0.0)

    @pl.when(not_last)
    def _():
        send_fields[0][0].start()

    @pl.when(not_first)
    def _():
        send_fields[0][1].start()

    inverse = jnp.where(column <= row, fac[:, states:], 0.0)
    turned = (((1,), (1,)), ((), ()))
    low_out[...] = lax.dot_general(site[1], inverse, turned, precision=highest, preferred_element_type=f32)

    @pl.when(not_first)
    def _():
        send_low.start()

    up_out[...] = lax.dot_general(site[0], inverse, turned, precision=highest, preferred_element_type=f32)
    store_up = pltpu.make_async_copy(up_out, out_hbm.at[0, 0], local_sem.at[3])
    store_up.start()

    @pl.when(not_first)
    def _():
        send_down.wait_recv()

    @pl.when(not_last)
    def _():
        send_up.wait_recv()

    def split_moved(a, carry):
        store_split(right_s, a, right_f[a])
        return carry

    lax.fori_loop(0, moved, split_moved, 0)

    def add_channels(field, start, stop):
        high, low_part = split_2(field)
        group = 2 if (stop - start) % 2 == 0 else 1

        def some(g, carry):
            total = acc[...]
            for k in range(group):
                a = start + g * group + k
                r_high, r_low = right_s[0, a], right_s[1, a]
                l_high, l_low = left_s[0, a], left_s[1, a]
                middle = dot(high, r_high) + dot(high, r_low) + dot(low_part, r_high)
                m_high, m_low = split_2(middle)
                total = total + dot(l_high, m_high) + dot(l_high, m_low) + dot(l_low, m_high)
            acc[...] = total
            return carry

        lax.fori_loop(0, (stop - start) // group, some, 0)

    def operator(t):
        acc[...] = jnp.zeros_like(acc)
        add_channels(fields[t][...], moved, channels)

        @pl.when(not_first)
        def _():
            send_fields[t][0].wait_recv()

        add_channels(field_in[t, 0], 0, W_DN)

        @pl.when(not_last)
        def _():
            send_fields[t][1].wait_recv()

        add_channels(field_in[t, 1], W_DN, moved)

    def reductions(t):
        for step in range(1, count):
            peer = lax.rem(me + step, count)
            yield pltpu.make_async_remote_copy(
                src_ref=red_own.at[t], dst_ref=red_in.at[t, step],
                send_sem=red_send.at[t, step], recv_sem=red_recv.at[t, step],
                device_id={"row": peer}, device_id_type=MESH,
            )

    operator(0)
    applied[...] = jnp.where(live_pair, acc[...], 0.0)

    @pl.when(not_last)
    def _():
        send_fields[1][0].start()

    @pl.when(not_first)
    def _():
        send_fields[1][1].start()

    red_own[0, :8] = tile_sum(bond[...] * bond[...])
    red_own[0, 8:] = tile_sum(bond[...] * applied[...])
    first_sums = list(reductions(0))
    for one in first_sums:
        one.start()

    operator(1)

    def collect(t, copies):
        total = red_own[t]
        for step, one in enumerate(copies, 1):
            one.wait_recv()
            total = total + red_in[t, step]
        return total

    total = collect(0, first_sums)
    start_norm = full_sum(total[:8])
    energy = full_sum(total[8:]) / start_norm
    shifted = applied[...] - energy * bond[...]
    second = jnp.where(live_pair, acc[...], 0.0) - energy * applied[...] - energy * shifted
    acc[...] = bond[...] + TAU * shifted + (0.5 * TAU * TAU) * second
    red_own[1, :8] = tile_sum(acc[...] * acc[...])
    red_own[1, 8:] = jnp.zeros((8, 128), f32)
    second_sums = list(reductions(1))
    for one in second_sums:
        one.start()

    @pl.when(not_last)
    def _():
        for one in (send_site, send_down, send_fields[0][0], send_fields[1][0]):
            one.wait_send()
        send_low.wait_recv()

    @pl.when(not_first)
    def _():
        for one in (send_up, send_low, send_fields[0][1], send_fields[1][1]):
            one.wait_send()

    @pl.when(me == count - 1)
    def _():
        low[...] = jnp.zeros_like(low)
        clear = pltpu.make_async_copy(low, out_hbm.at[0, 1], local_sem.at[4])
        clear.start()
        clear.wait()

    store_up.wait()
    final_norm = full_sum(collect(1, second_sums)[:8])
    bond_out[0] = acc[...] * jnp.sqrt(start_norm / final_norm)
    for one in first_sums + second_sums:
        one.wait_send()


def on_device(site_tensor, left_env, right_env, sector_size):
    states = site_tensor.shape[-1]
    channels = left_env.shape[1]
    count = lax.axis_size("row")
    block = (states, states)
    anywhere = pl.BlockSpec(memory_space=pl.ANY)
    return pl.pallas_call(
        kernel,
        out_shape=(
            jax.ShapeDtypeStruct(site_tensor.shape, f32),
            jax.ShapeDtypeStruct((1,) + block, f32),
        ),
        in_specs=[pl.BlockSpec(memory_space=pltpu.SMEM), anywhere, anywhere, anywhere],
        out_specs=(anywhere, pl.BlockSpec(memory_space=pltpu.VMEM)),
        scratch_shapes=[
            pltpu.VMEM((2,) + block, f32),
            pltpu.VMEM(block, f32),
            pltpu.VMEM((channels,) + block, f32),
            pltpu.VMEM((channels,) + block, f32),
            pltpu.VMEM((2, channels) + block, bf16),
            pltpu.VMEM((2, channels) + block, bf16),
            pltpu.VMEM((states, 2 * states), f32),
            pltpu.VMEM((states, 2 * states), f32),
            pltpu.VMEM(block, f32),
            pltpu.VMEM(block, f32),
            pltpu.VMEM(block, f32),
            pltpu.VMEM((2, 2) + block, f32),
            pltpu.VMEM(block, f32),
            pltpu.VMEM(block, f32),
            pltpu.VMEM((2, count, 16, 128), f32),
            pltpu.VMEM((2, 16, 128), f32),
            pltpu.SemaphoreType.DMA((5,)),
            pltpu.SemaphoreType.DMA((8,)),
            pltpu.SemaphoreType.DMA((8,)),
            pltpu.SemaphoreType.DMA((2, count)),
            pltpu.SemaphoreType.DMA((2, count)),
        ],
        compiler_params=pltpu.CompilerParams(
            collective_id=0, has_side_effects=True, vmem_limit_bytes=56 * 1024 * 1024
        ),
        name="bond_update",
    )(sector_size, site_tensor, left_env, right_env)


def solution(mesh):
    placed = (
        P(("real", "row"), None, None, None),
        P(("real", "row"), None, None, None),
        P(("real", "row"), None, None, None),
        P("real"),
    )
    return jax.shard_map(
        on_device,
        mesh=mesh,
        in_specs=placed,
        out_specs=(P(("real", "row"), None, None, None), P(("real", "row"), None, None)),
        check_vma=False,
    )
```

```python
import functools

import jax
import jax.numpy as jnp
from jax import lax
from jax.experimental import pallas as pl
from jax.experimental.pallas import tpu as pltpu
from jax.sharding import PartitionSpec as P

W_DN = 4
W_UP = 4
PANEL = 16
TAU = 0.15
highest = lax.Precision.HIGHEST
f32 = jnp.float32
bf16 = jnp.bfloat16
MESH = pl.DeviceIdType.MESH


def dot(a, b):
    return jnp.dot(a, b, preferred_element_type=f32)


def split_2(value):
    high = value.astype(bf16)
    return high, (value - high.astype(f32)).astype(bf16)


def split_3(value):
    high = value.astype(bf16)
    rest = value - high.astype(f32)
    middle = rest.astype(bf16)
    return high, middle, (rest - middle.astype(f32)).astype(bf16)


def store_split(pair_ref, index, value):
    high, low = split_2(value)
    pair_ref[0, index] = high
    pair_ref[1, index] = low


def tile_sum(value):
    rows, columns = value.shape
    summed = jnp.sum(value.reshape(rows // 8, 8, columns), axis=0)
    total = summed[:, :128]
    for start in range(128, columns, 128):
        total = total + summed[:, start : start + 128]
    return total


def full_sum(tile):
    return jnp.sum(jnp.sum(tile, axis=0, keepdims=True), axis=1, keepdims=True)


def panel_step(p, lo, hi, states, aug_ref, out_ref):
    base = pl.multiple_of(p * PANEL, PANEL)
    row_id = lax.broadcasted_iota(jnp.int32, (PANEL, 128), 0)
    offset = lax.rem(p * PANEL, 128)
    diag = aug_ref[pl.ds(base, PANEL), lo : lo + 128]
    diag = pltpu.roll(diag, lax.rem(128 - offset, 128), 1)
    columns = [jnp.broadcast_to(diag[:, r : r + 1], (PANEL, 128)) for r in range(PANEL)]
    tiles = [aug_ref[pl.ds(base, PANEL), t : t + 128] for t in range(lo, hi, 128)]
    scale = jnp.zeros((PANEL, 128), f32)
    for r in range(PANEL):
        inverse = lax.rsqrt(columns[r][r : r + 1, :])
        scale = jnp.where(row_id == r, inverse, scale)
        multiplier = columns[r] * inverse
        below = jnp.where(row_id > r, multiplier, 0.0)
        for s in range(r + 1, PANEL):
            columns[s] = columns[s] - below * multiplier[s : s + 1, :]
        if r < PANEL - 1:
            tiles = [tile - below * (tile[r : r + 1, :] * inverse) for tile in tiles]
    tiles = [tile * scale for tile in tiles]
    for t, tile in zip(range(lo, hi, 128), tiles):
        out_ref[pl.ds(base, PANEL), t : t + 128] = tile
    panel = jnp.concatenate(tiles, 1)
    q1, q2, q3 = split_3(panel)
    p1, p2, p3 = (q[:, : states - lo] for q in (q1, q2, q3))
    left = jnp.concatenate([p1, p1, p2, p2, p1, p3], 0)
    right = jnp.concatenate([q1, q2, q1, q2, q3, q1], 0)
    update = lax.dot_general(left, right, (((0,), (0,)), ((), ())), preferred_element_type=f32)
    aug_ref[lo:states, lo:hi] -= update


def kernel(
    size_ref, site_hbm, left_hbm, right_hbm,
    out_hbm, bond_out,
    site, low, left_f, right_f, left_s, right_s, aug, fac, packed, bond, applied, acc, field_in, field_s, low_out, up_out,
    red_in, red_own, local_sem, send_sem, recv_sem, red_send, red_recv,
):
    count = lax.axis_size("row")
    me = lax.axis_index("row")
    states = site.shape[-1]
    channels = left_f.shape[0]
    moved = W_DN + W_UP
    not_first, not_last = me > 0, me < count - 1

    loads = [
        pltpu.make_async_copy(site_hbm.at[0], site, local_sem.at[0]),
        pltpu.make_async_copy(left_hbm.at[0], left_f, local_sem.at[1]),
        pltpu.make_async_copy(right_hbm.at[0, moved:], right_f.at[moved:], local_sem.at[2]),
    ]
    for load in loads:
        load.start()

    barrier = pltpu.get_barrier_semaphore()
    for step in range(1, count):
        peer = lax.rem(me + step, count)
        pl.semaphore_signal(barrier, inc=1, device_id={"row": peer}, device_id_type=MESH)
    pl.semaphore_wait(barrier, count - 1)

    def remote(source, target, slot, peer):
        return pltpu.make_async_remote_copy(
            src_ref=source, dst_ref=target, send_sem=send_sem.at[slot], recv_sem=recv_sem.at[slot],
            device_id={"row": peer}, device_id_type=MESH,
        )

    to_right, to_left = jnp.minimum(me + 1, count - 1), jnp.maximum(me - 1, 0)
    half = states // 2
    send_site = remote(site_hbm.at[0, 1], low, 0, to_right)
    send_down = [remote(right_hbm.at[0, a], right_f.at[a], 1 + a, to_right) for a in range(W_DN)]
    send_up = [remote(right_hbm.at[0, a], right_f.at[a], 1 + a, to_left) for a in range(W_DN, moved)]
    send_bond_right = [
        remote(packed.at[:half], field_in.at[0, 0, :half], moved + 1, to_right),
        remote(packed.at[half:, half:], field_in.at[0, 0, half:, half:], moved + 2, to_right),
    ]
    send_bond_left = remote(packed, field_in.at[0, 1], moved + 3, to_left)
    send_applied_right = remote(applied, field_in.at[1, 0], moved + 4, to_right)
    send_applied_left = remote(applied, field_in.at[1, 1], moved + 5, to_left)
    rightward = [send_site] + send_down + send_bond_right + [send_applied_right]
    leftward = send_up + [send_bond_left, send_applied_left]
    early_down, early_up = W_DN // 2, W_UP // 2

    @pl.when(not_last)
    def _():
        send_site.start()

    @pl.when(me == 0)
    def _():
        low[...] = jnp.zeros_like(low)
        right_f[:W_DN] = jnp.zeros((W_DN, states, states), f32)
        field_in[:, 0] = jnp.zeros((2, states, states), f32)

    @pl.when(me == count - 1)
    def _():
        right_f[W_DN:moved] = jnp.zeros((W_UP, states, states), f32)
        field_in[:, 1] = jnp.zeros((2, states, states), f32)

    size = size_ref[me]
    size_before = size_ref[to_left]
    size_after = size_ref[to_right]
    row = lax.broadcasted_iota(jnp.int32, (states, states), 0)
    column = lax.broadcasted_iota(jnp.int32, (states, states), 1)
    live_pair = (row < size) & (column < size)
    gram_dims = (((0,), (0,)), ((), ()))
    loads[0].wait()
    upper = jnp.where(live_pair, site[0], 0.0)
    site[0] = upper
    gram = lax.dot_general(upper, upper, gram_dims, precision=highest, preferred_element_type=f32)
    gram = gram + jnp.where((row == column) & (row >= size), 1.0, 0.0)
    aug[:, states:] = jnp.where(row == column, 1.0, 0.0).astype(f32)

    @pl.when(not_last)
    def _():
        send_site.wait_send()
        for one in send_down[:early_down]:
            one.start()

    @pl.when(not_first)
    def _():
        for one in send_up[:early_up]:
            one.start()
        send_site.wait_recv()

    lower = jnp.where((row < size_before) & (column < size), low[...], 0.0)
    aug[:, :states] = gram + lax.dot_general(lower, lower, gram_dims, precision=highest, preferred_element_type=f32)
    fac[...] = jnp.zeros_like(fac)
    loads[1].wait()
    loads[2].wait()

    halves = half // PANEL

    def first_half(p, carry):
        panel_step(p, 0, states + half, states, aug, fac)
        store_split(left_s, p, left_f[p])
        return carry

    def second_half(p, carry):
        panel_step(p, half, 2 * states, states, aug, fac)
        other = jnp.minimum(p, channels - 1)
        store_split(left_s, other, left_f[other])
        mine = jnp.minimum(p - halves + moved, channels - 1)
        store_split(right_s, mine, right_f[mine])
        return carry

    lax.fori_loop(0, halves, first_half, 0)
    lax.fori_loop(halves, 2 * halves, second_half, 0)

    packed[...] = jnp.where(column >= row, fac[:, :states], fac[:, states:])

    @pl.when(not_last)
    def _():
        for one in send_bond_right + send_down[early_down:]:
            one.start()

    @pl.when(not_first)
    def _():
        for one in [send_bond_left] + send_up[early_up:]:
            one.start()

    bond[...] = jnp.where(live_pair & (column >= row), fac[:, :states], 0.0)
    inverse = jnp.where(column <= row, fac[:, states:], 0.0)
    turned = (((1,), (1,)), ((), ()))
    up_out[...] = lax.dot_general(site[0], inverse, turned, precision=highest, preferred_element_type=f32)
    store_up = pltpu.make_async_copy(up_out, out_hbm.at[0, 0], local_sem.at[3])
    store_up.start()

    def put_field(which, value):
        field_s[which, 0], field_s[which, 1] = split_2(value)

    def add_terms(total, which, a):
        high, low_part = field_s[which, 0], field_s[which, 1]
        r_high, r_low = right_s[0, a], right_s[1, a]
        l_high, l_low = left_s[0, a], left_s[1, a]
        middle = dot(high, r_high) + dot(high, r_low) + dot(low_part, r_high)
        m_high, m_low = split_2(middle)
        return total + dot(l_high, m_high) + dot(l_high, m_low) + dot(l_low, m_high)

    def add_range(which, start, stop):
        group = 2 if (stop - start) % 2 == 0 else 1

        def some(g, carry):
            total = acc[...]
            for k in range(group):
                total = add_terms(total, which, start + g * group + k)
            acc[...] = total
            return carry

        lax.fori_loop(0, (stop - start) // group, some, 0)

    def take_moved(down, up):
        @pl.when(not_first)
        def _():
            for a in down:
                send_down[a].wait_recv()

        @pl.when(not_last)
        def _():
            for a in up:
                send_up[a - W_DN].wait_recv()

        for a in (*down, *up):
            store_split(right_s, a, right_f[a])

    acc[...] = jnp.zeros_like(acc)
    put_field(0, bond[...])
    add_range(0, moved, channels)
    take_moved(range(early_down), range(W_DN, W_DN + early_up))

    @pl.when(not_first)
    def _():
        for one in send_bond_right:
            one.wait_recv()

    put_field(1, jnp.where((column >= row) & (row < size_before) & (column < size_before), field_in[0, 0], 0.0))
    add_range(1, 0, early_down)

    @pl.when(not_last)
    def _():
        send_bond_left.wait_recv()

    near = field_in[0, 1]
    put_field(2, jnp.where((column >= row) & (row < size_after) & (column < size_after), near, 0.0))
    add_range(2, W_DN, W_DN + early_up)
    near_inverse = jnp.where(column < row, near, jnp.where(column == row, 1.0 / near, 0.0))
    outer = jnp.where((row < size) & (column < size_after), site[1], 0.0)
    outer = lax.dot_general(outer, near_inverse, turned, precision=highest, preferred_element_type=f32)
    low_out[...] = jnp.where(not_last, outer, 0.0)
    store_low = pltpu.make_async_copy(low_out, out_hbm.at[0, 1], local_sem.at[4])
    store_low.start()
    for k in range(max(W_DN - early_down, W_UP - early_up)):
        down = [early_down + k] if early_down + k < W_DN else []
        up = [W_DN + early_up + k] if early_up + k < W_UP else []
        take_moved(down, up)
        total = acc[...]
        for which, group in ((1, down), (2, up)):
            for a in group:
                total = add_terms(total, which, a)
        acc[...] = total

    def reductions(t):
        for step in range(1, count):
            peer = lax.rem(me + step, count)
            yield pltpu.make_async_remote_copy(
                src_ref=red_own.at[t], dst_ref=red_in.at[t, step],
                send_sem=red_send.at[t, step], recv_sem=red_recv.at[t, step],
                device_id={"row": peer}, device_id_type=MESH,
            )

    applied[...] = jnp.where(live_pair, acc[...], 0.0)

    @pl.when(not_last)
    def _():
        send_applied_right.start()

    @pl.when(not_first)
    def _():
        send_applied_left.start()

    red_own[0, :8] = tile_sum(bond[...] * bond[...])
    red_own[0, 8:] = tile_sum(bond[...] * applied[...])
    first_sums = list(reductions(0))
    for one in first_sums:
        one.start()

    acc[...] = jnp.zeros_like(acc)
    put_field(0, applied[...])
    add_range(0, moved, channels)

    @pl.when(not_first)
    def _():
        send_applied_right.wait_recv()

    put_field(1, field_in[1, 0])
    add_range(1, 0, W_DN)

    @pl.when(not_last)
    def _():
        send_applied_left.wait_recv()

    put_field(2, field_in[1, 1])
    add_range(2, W_DN, moved)

    def collect(t, copies):
        total = red_own[t]
        for step, one in enumerate(copies, 1):
            one.wait_recv()
            total = total + red_in[t, step]
        return total

    total = collect(0, first_sums)
    start_norm = full_sum(total[:8])
    energy = full_sum(total[8:]) / start_norm
    shifted = applied[...] - energy * bond[...]
    second = jnp.where(live_pair, acc[...], 0.0) - energy * applied[...] - energy * shifted
    acc[...] = bond[...] + TAU * shifted + (0.5 * TAU * TAU) * second
    red_own[1, :8] = tile_sum(acc[...] * acc[...])
    red_own[1, 8:] = jnp.zeros((8, 128), f32)
    second_sums = list(reductions(1))
    for one in second_sums:
        one.start()

    @pl.when(not_last)
    def _():
        for one in rightward[1:]:
            one.wait_send()

    @pl.when(not_first)
    def _():
        for one in leftward:
            one.wait_send()

    store_low.wait()
    store_up.wait()
    final_norm = full_sum(collect(1, second_sums)[:8])
    bond_out[0] = acc[...] * jnp.sqrt(start_norm / final_norm)
    for one in first_sums + second_sums:
        one.wait_send()


def on_device(site_tensor, left_env, right_env, sector_size):
    states = site_tensor.shape[-1]
    channels = left_env.shape[1]
    count = lax.axis_size("row")
    block = (states, states)
    anywhere = pl.BlockSpec(memory_space=pl.ANY)
    return pl.pallas_call(
        kernel,
        out_shape=(
            jax.ShapeDtypeStruct(site_tensor.shape, f32),
            jax.ShapeDtypeStruct((1,) + block, f32),
        ),
        in_specs=[pl.BlockSpec(memory_space=pltpu.SMEM), anywhere, anywhere, anywhere],
        out_specs=(anywhere, pl.BlockSpec(memory_space=pltpu.VMEM)),
        scratch_shapes=[
            pltpu.VMEM((2,) + block, f32),
            pltpu.VMEM(block, f32),
            pltpu.VMEM((channels,) + block, f32),
            pltpu.VMEM((channels,) + block, f32),
            pltpu.VMEM((2, channels) + block, bf16),
            pltpu.VMEM((2, channels) + block, bf16),
            pltpu.VMEM((states, 2 * states), f32),
            pltpu.VMEM((states, 2 * states), f32),
            pltpu.VMEM(block, f32),
            pltpu.VMEM(block, f32),
            pltpu.VMEM(block, f32),
            pltpu.VMEM(block, f32),
            pltpu.VMEM((2, 2) + block, f32),
            pltpu.VMEM((3, 2) + block, bf16),
            pltpu.VMEM(block, f32),
            pltpu.VMEM(block, f32),
            pltpu.VMEM((2, count, 16, 128), f32),
            pltpu.VMEM((2, 16, 128), f32),
            pltpu.SemaphoreType.DMA((5,)),
            pltpu.SemaphoreType.DMA((W_DN + W_UP + 6,)),
            pltpu.SemaphoreType.DMA((W_DN + W_UP + 6,)),
            pltpu.SemaphoreType.DMA((2, count)),
            pltpu.SemaphoreType.DMA((2, count)),
        ],
        compiler_params=pltpu.CompilerParams(
            collective_id=0, has_side_effects=True, vmem_limit_bytes=56 * 1024 * 1024
        ),
        name="bond_update",
    )(sector_size, site_tensor, left_env, right_env)


def solution(mesh):
    placed = (
        P(("real", "row"), None, None, None),
        P(("real", "row"), None, None, None),
        P(("real", "row"), None, None, None),
        P("real"),
    )
    return jax.shard_map(
        on_device,
        mesh=mesh,
        in_specs=placed,
        out_specs=(P(("real", "row"), None, None, None), P(("real", "row"), None, None)),
        check_vma=False,
    )
```

```python
import functools

import jax
import jax.numpy as jnp
from jax import lax
from jax.experimental import pallas as pl
from jax.experimental.pallas import tpu as pltpu
from jax.sharding import PartitionSpec as P

W_DN = 4
W_UP = 4
PANEL = 16
TAU = 0.15
highest = lax.Precision.HIGHEST
f32 = jnp.float32
bf16 = jnp.bfloat16
MESH = pl.DeviceIdType.MESH


def dot(a, b):
    return jnp.dot(a, b, preferred_element_type=f32)


def split_2(value):
    high = value.astype(bf16)
    return high, (value - high.astype(f32)).astype(bf16)


def split_3(value):
    high = value.astype(bf16)
    rest = value - high.astype(f32)
    middle = rest.astype(bf16)
    return high, middle, (rest - middle.astype(f32)).astype(bf16)


def store_split(pair_ref, index, value):
    high, low = split_2(value)
    pair_ref[0, index] = high
    pair_ref[1, index] = low


def tile_sum(value):
    rows, columns = value.shape
    summed = jnp.sum(value.reshape(rows // 8, 8, columns), axis=0)
    total = summed[:, :128]
    for start in range(128, columns, 128):
        total = total + summed[:, start : start + 128]
    return total


def full_sum(tile):
    return jnp.sum(jnp.sum(tile, axis=0, keepdims=True), axis=1, keepdims=True)


def panel_step(p, lo, hi, states, aug_ref, out_ref):
    base = pl.multiple_of(p * PANEL, PANEL)
    row_id = lax.broadcasted_iota(jnp.int32, (PANEL, 128), 0)
    offset = lax.rem(p * PANEL, 128)
    diag = aug_ref[pl.ds(base, PANEL), lo : lo + 128]
    diag = pltpu.roll(diag, lax.rem(128 - offset, 128), 1)
    columns = [jnp.broadcast_to(diag[:, r : r + 1], (PANEL, 128)) for r in range(PANEL)]
    tiles = [aug_ref[pl.ds(base, PANEL), t : t + 128] for t in range(lo, hi, 128)]
    scale = jnp.zeros((PANEL, 128), f32)
    for r in range(PANEL):
        inverse = lax.rsqrt(columns[r][r : r + 1, :])
        scale = jnp.where(row_id == r, inverse, scale)
        multiplier = columns[r] * inverse
        below = jnp.where(row_id > r, multiplier, 0.0)
        for s in range(r + 1, PANEL):
            columns[s] = columns[s] - below * multiplier[s : s + 1, :]
        if r < PANEL - 1:
            tiles = [tile - below * (tile[r : r + 1, :] * inverse) for tile in tiles]
    tiles = [tile * scale for tile in tiles]
    for t, tile in zip(range(lo, hi, 128), tiles):
        out_ref[pl.ds(base, PANEL), t : t + 128] = tile
    panel = jnp.concatenate(tiles, 1)
    q1, q2, q3 = split_3(panel)
    p1, p2, p3 = (q[:, : states - lo] for q in (q1, q2, q3))
    left = jnp.concatenate([p1, p1, p2, p2, p1, p3], 0)
    right = jnp.concatenate([q1, q2, q1, q2, q3, q1], 0)
    update = lax.dot_general(left, right, (((0,), (0,)), ((), ())), preferred_element_type=f32)
    aug_ref[lo:states, lo:hi] -= update


def kernel(
    size_ref, site_hbm, left_hbm, right_hbm,
    left_out, bond_out,
    site, low, left_f, right_f, left_s, right_s, aug, fac, packed, bond, applied, acc, field_in, field_s,
    red_in, red_own, local_sem, send_sem, recv_sem, red_send, red_recv,
):
    count = lax.axis_size("row")
    me = lax.axis_index("row")
    states = site.shape[-1]
    channels = left_f.shape[0]
    moved = W_DN + W_UP
    not_first, not_last = me > 0, me < count - 1

    loads = [
        pltpu.make_async_copy(site_hbm.at[0], site, local_sem.at[0]),
        pltpu.make_async_copy(left_hbm.at[0], left_f, local_sem.at[1]),
        pltpu.make_async_copy(right_hbm.at[0, moved:], right_f.at[moved:], local_sem.at[2]),
    ]
    for load in loads:
        load.start()

    barrier = pltpu.get_barrier_semaphore()
    for step in range(1, count):
        peer = lax.rem(me + step, count)
        pl.semaphore_signal(barrier, inc=1, device_id={"row": peer}, device_id_type=MESH)
    pl.semaphore_wait(barrier, count - 1)

    def remote(source, target, slot, peer):
        return pltpu.make_async_remote_copy(
            src_ref=source, dst_ref=target, send_sem=send_sem.at[slot], recv_sem=recv_sem.at[slot],
            device_id={"row": peer}, device_id_type=MESH,
        )

    to_right, to_left = jnp.minimum(me + 1, count - 1), jnp.maximum(me - 1, 0)
    half = states // 2
    send_site = remote(site_hbm.at[0, 1], low, 0, to_right)
    send_down = [remote(right_hbm.at[0, a], right_f.at[a], 1 + a, to_right) for a in range(W_DN)]
    send_up = [remote(right_hbm.at[0, a], right_f.at[a], 1 + a, to_left) for a in range(W_DN, moved)]
    send_bond_right = [
        remote(packed.at[:half], field_in.at[0, 0, :half], moved + 1, to_right),
        remote(packed.at[half:, half:], field_in.at[0, 0, half:, half:], moved + 2, to_right),
    ]
    send_bond_left = remote(packed, field_in.at[0, 1], moved + 3, to_left)
    send_applied_right = remote(applied, field_in.at[1, 0], moved + 4, to_right)
    send_applied_left = remote(applied, field_in.at[1, 1], moved + 5, to_left)
    rightward = [send_site] + send_down + send_bond_right + [send_applied_right]
    leftward = send_up + [send_bond_left, send_applied_left]
    early_down, early_up = W_DN // 2, W_UP // 2

    @pl.when(not_last)
    def _():
        send_site.start()

    @pl.when(me == 0)
    def _():
        low[...] = jnp.zeros_like(low)
        right_f[:W_DN] = jnp.zeros((W_DN, states, states), f32)
        field_in[:, 0] = jnp.zeros((2, states, states), f32)

    @pl.when(me == count - 1)
    def _():
        right_f[W_DN:moved] = jnp.zeros((W_UP, states, states), f32)
        field_in[:, 1] = jnp.zeros((2, states, states), f32)

    size = size_ref[me]
    size_before = size_ref[to_left]
    size_after = size_ref[to_right]
    row = lax.broadcasted_iota(jnp.int32, (states, states), 0)
    column = lax.broadcasted_iota(jnp.int32, (states, states), 1)
    live_pair = (row < size) & (column < size)
    gram_dims = (((0,), (0,)), ((), ()))
    loads[0].wait()
    upper = jnp.where(live_pair, site[0], 0.0)
    site[0] = upper
    gram = lax.dot_general(upper, upper, gram_dims, precision=highest, preferred_element_type=f32)
    gram = gram + jnp.where((row == column) & (row >= size), 1.0, 0.0)
    aug[:, states:] = jnp.where(row == column, 1.0, 0.0).astype(f32)

    @pl.when(not_last)
    def _():
        send_site.wait_send()
        for one in send_down[:early_down]:
            one.start()

    @pl.when(not_first)
    def _():
        for one in send_up[:early_up]:
            one.start()
        send_site.wait_recv()

    lower = jnp.where((row < size_before) & (column < size), low[...], 0.0)
    aug[:, :states] = gram + lax.dot_general(lower, lower, gram_dims, precision=highest, preferred_element_type=f32)
    fac[...] = jnp.zeros_like(fac)
    loads[1].wait()
    loads[2].wait()

    halves = half // PANEL

    def first_half(p, carry):
        panel_step(p, 0, states + half, states, aug, fac)
        store_split(left_s, p, left_f[p])
        return carry

    def second_half(p, carry):
        panel_step(p, half, 2 * states, states, aug, fac)
        other = jnp.minimum(p, channels - 1)
        store_split(left_s, other, left_f[other])
        mine = jnp.minimum(p - halves + moved, channels - 1)
        store_split(right_s, mine, right_f[mine])
        return carry

    lax.fori_loop(0, halves, first_half, 0)
    lax.fori_loop(halves, 2 * halves, second_half, 0)

    packed[...] = jnp.where(column >= row, fac[:, :states], fac[:, states:])

    @pl.when(not_last)
    def _():
        for one in send_bond_right + send_down[early_down:]:
            one.start()

    @pl.when(not_first)
    def _():
        for one in [send_bond_left] + send_up[early_up:]:
            one.start()

    bond[...] = jnp.where(live_pair & (column >= row), fac[:, :states], 0.0)
    inverse = jnp.where(column <= row, fac[:, states:], 0.0)
    turned = (((1,), (1,)), ((), ()))
    left_out[0] = lax.dot_general(site[0], inverse, turned, precision=highest, preferred_element_type=f32)

    def put_field(which, value):
        field_s[which, 0], field_s[which, 1] = split_2(value)

    def add_terms(total, which, a):
        high, low_part = field_s[which, 0], field_s[which, 1]
        r_high, r_low = right_s[0, a], right_s[1, a]
        l_high, l_low = left_s[0, a], left_s[1, a]
        middle = dot(high, r_high) + dot(high, r_low) + dot(low_part, r_high)
        m_high, m_low = split_2(middle)
        return total + dot(l_high, m_high) + dot(l_high, m_low) + dot(l_low, m_high)

    def add_range(which, start, stop):
        group = 2 if (stop - start) % 2 == 0 else 1

        def some(g, carry):
            total = acc[...]
            for k in range(group):
                total = add_terms(total, which, start + g * group + k)
            acc[...] = total
            return carry

        lax.fori_loop(0, (stop - start) // group, some, 0)

    def take_moved(down, up):
        @pl.when(not_first)
        def _():
            for a in down:
                send_down[a].wait_recv()

        @pl.when(not_last)
        def _():
            for a in up:
                send_up[a - W_DN].wait_recv()

        for a in (*down, *up):
            store_split(right_s, a, right_f[a])

    acc[...] = jnp.zeros_like(acc)
    put_field(0, bond[...])
    add_range(0, moved, channels)
    take_moved(range(early_down), range(W_DN, W_DN + early_up))

    @pl.when(not_first)
    def _():
        for one in send_bond_right:
            one.wait_recv()

    put_field(1, jnp.where((column >= row) & (row < size_before) & (column < size_before), field_in[0, 0], 0.0))
    add_range(1, 0, early_down)

    @pl.when(not_last)
    def _():
        send_bond_left.wait_recv()

    near = field_in[0, 1]
    put_field(2, jnp.where((column >= row) & (row < size_after) & (column < size_after), near, 0.0))
    add_range(2, W_DN, W_DN + early_up)
    near_inverse = jnp.where(column < row, near, jnp.where(column == row, 1.0 / near, 0.0))
    outer = jnp.where((row < size) & (column < size_after), site[1], 0.0)
    outer = lax.dot_general(outer, near_inverse, turned, precision=highest, preferred_element_type=f32)
    left_out[1] = jnp.where(not_last, outer, 0.0)
    for k in range(max(W_DN - early_down, W_UP - early_up)):
        down = [early_down + k] if early_down + k < W_DN else []
        up = [W_DN + early_up + k] if early_up + k < W_UP else []
        take_moved(down, up)
        total = acc[...]
        for which, group in ((1, down), (2, up)):
            for a in group:
                total = add_terms(total, which, a)
        acc[...] = total

    def reductions(t):
        for step in range(1, count):
            peer = lax.rem(me + step, count)
            yield pltpu.make_async_remote_copy(
                src_ref=red_own.at[t], dst_ref=red_in.at[t, step],
                send_sem=red_send.at[t, step], recv_sem=red_recv.at[t, step],
                device_id={"row": peer}, device_id_type=MESH,
            )

    applied[...] = jnp.where(live_pair, acc[...], 0.0)

    @pl.when(not_last)
    def _():
        send_applied_right.start()

    @pl.when(not_first)
    def _():
        send_applied_left.start()

    red_own[0, :8] = tile_sum(bond[...] * bond[...])
    red_own[0, 8:] = tile_sum(bond[...] * applied[...])
    first_sums = list(reductions(0))
    for one in first_sums:
        one.start()

    acc[...] = jnp.zeros_like(acc)
    put_field(0, applied[...])
    add_range(0, moved, channels)

    @pl.when(not_first)
    def _():
        send_applied_right.wait_recv()

    put_field(1, field_in[1, 0])
    add_range(1, 0, W_DN)

    @pl.when(not_last)
    def _():
        send_applied_left.wait_recv()

    put_field(2, field_in[1, 1])
    add_range(2, W_DN, moved)

    def collect(t, copies):
        total = red_own[t]
        for step, one in enumerate(copies, 1):
            one.wait_recv()
            total = total + red_in[t, step]
        return total

    total = collect(0, first_sums)
    start_norm = full_sum(total[:8])
    energy = full_sum(total[8:]) / start_norm
    shifted = applied[...] - energy * bond[...]
    second = jnp.where(live_pair, acc[...], 0.0) - energy * applied[...] - energy * shifted
    acc[...] = bond[...] + TAU * shifted + (0.5 * TAU * TAU) * second
    red_own[1, :8] = tile_sum(acc[...] * acc[...])
    red_own[1, 8:] = jnp.zeros((8, 128), f32)
    second_sums = list(reductions(1))
    for one in second_sums:
        one.start()

    @pl.when(not_last)
    def _():
        for one in rightward[1:]:
            one.wait_send()

    @pl.when(not_first)
    def _():
        for one in leftward:
            one.wait_send()

    final_norm = full_sum(collect(1, second_sums)[:8])
    bond_out[...] = acc[...] * jnp.sqrt(start_norm / final_norm)
    for one in first_sums + second_sums:
        one.wait_send()


def write_out(left, bond, left_hbm, bond_hbm, sem):
    stores = [
        pltpu.make_async_copy(left, left_hbm.at[0], sem.at[0]),
        pltpu.make_async_copy(bond, bond_hbm.at[0], sem.at[1]),
    ]
    for store in stores:
        store.start()
    for store in stores:
        store.wait()


def on_device(site_tensor, left_env, right_env, sector_size):
    states = site_tensor.shape[-1]
    channels = left_env.shape[1]
    count = lax.axis_size("row")
    block = (states, states)
    anywhere = pl.BlockSpec(memory_space=pl.ANY)
    inside = pl.BlockSpec(memory_space=pltpu.VMEM)
    left_out, bond_out = pl.pallas_call(
        kernel,
        out_shape=(
            pltpu.VMEM((2,) + block, f32),
            pltpu.VMEM(block, f32),
        ),
        in_specs=[pl.BlockSpec(memory_space=pltpu.SMEM)] + [pl.BlockSpec(memory_space=pltpu.HBM)] * 3,
        out_specs=(inside, inside),
        scratch_shapes=[
            pltpu.VMEM((2,) + block, f32),
            pltpu.VMEM(block, f32),
            pltpu.VMEM((channels,) + block, f32),
            pltpu.VMEM((channels,) + block, f32),
            pltpu.VMEM((2, channels) + block, bf16),
            pltpu.VMEM((2, channels) + block, bf16),
            pltpu.VMEM((states, 2 * states), f32),
            pltpu.VMEM((states, 2 * states), f32),
            pltpu.VMEM(block, f32),
            pltpu.VMEM(block, f32),
            pltpu.VMEM(block, f32),
            pltpu.VMEM(block, f32),
            pltpu.VMEM((2, 2) + block, f32),
            pltpu.VMEM((3, 2) + block, bf16),
            pltpu.VMEM((2, count, 16, 128), f32),
            pltpu.VMEM((2, 16, 128), f32),
            pltpu.SemaphoreType.DMA((3,)),
            pltpu.SemaphoreType.DMA((W_DN + W_UP + 6,)),
            pltpu.SemaphoreType.DMA((W_DN + W_UP + 6,)),
            pltpu.SemaphoreType.DMA((2, count)),
            pltpu.SemaphoreType.DMA((2, count)),
        ],
        compiler_params=pltpu.CompilerParams(
            collective_id=0, has_side_effects=True, vmem_limit_bytes=60 * 1024 * 1024
        ),
        name="bond_update",
    )(sector_size, site_tensor, left_env, right_env)
    return pl.pallas_call(
        write_out,
        out_shape=(
            jax.ShapeDtypeStruct(site_tensor.shape, f32),
            jax.ShapeDtypeStruct((1,) + block, f32),
        ),
        in_specs=[inside, inside],
        out_specs=(anywhere, anywhere),
        scratch_shapes=[pltpu.SemaphoreType.DMA((2,))],
        compiler_params=pltpu.CompilerParams(vmem_limit_bytes=4 * 1024 * 1024),
        name="write_out",
    )(left_out, bond_out)


def solution(mesh):
    placed = (
        P(("real", "row"), None, None, None),
        P(("real", "row"), None, None, None),
        P(("real", "row"), None, None, None),
        P("real"),
    )
    return jax.shard_map(
        on_device,
        mesh=mesh,
        in_specs=placed,
        out_specs=(P(("real", "row"), None, None, None), P(("real", "row"), None, None)),
        check_vma=False,
    )
```
